32 devices in a mesh: unit: 4 (over z), lat: 2 (over y), lon: 2 (over core), lev: 2 (over x).
Axes of the slice: x: 2, y: 2, z: 4, core: 2. Of those that a mesh axis runs over, the one named last changes fastest.
Arguments:
- tracer: float32 [32, 128, 64, 128], P(('unit', 'lat'), 'lon', 'lev'), parts along dimension 0, may hold values from 0.2 to 1.8
- crowding: float32 [32, 128, 64, 128], P(('unit', 'lat'), 'lon', 'lev'), parts along dimension 0, may hold values from 0.5 to 2
Outputs:
- column_sum: float32 [32, 128, 64, 128], P(('unit', 'lat'), 'lon', 'lev'), parts along dimension 0
- tracer_end: float32 [32, 128, 64, 128], P(('unit', 'lat'), 'lon', 'lev'), parts along dimension 0
The draws below stay inside these ranges and needn't reach their ends.
There are 4 independent parts, one for each index of `unit`. The reference program is written for one: setup_inputs(seed, part) draws one part's arguments, and reference() takes and returns one part's arrays. A program takes and returns all parts, laid end to end along the dimension named above; each array names one. Nothing has to cross between parts.
All inputs are finite; a program needn't handle non-finite values.
Results may differ from the reference program's by a relative error of at most 0.00002.
Values sent between devices are 32-bit elements; how exact they have to be, the bound alone decides.
A program may use at most 128 MiB of HBM per device.

```python
import jax
import jax.numpy as jnp
from jax import lax

GRID_J = 8
GRID_I = 128
GRID_K = 64
LEVELS = 128
STEPS = 4


def steps_of(key, extent, pieces, low, top_value):
    level = 1.0
    for axis_at, shards_of in pieces:
        draws = jax.random.uniform(jax.random.fold_in(jax.random.fold_in(key, 6), axis_at), (shards_of,), jnp.float32, low / len(pieces), top_value / len(pieces))
        level = level * jnp.repeat(jnp.exp(draws), extent[axis_at] // shards_of).reshape((-1,) + (1,) * (len(extent) - 1 - axis_at))
    return level


def setup_inputs(seed: int = 0, part: int = 0) -> dict:
    key_of = jax.random.split(jax.random.key(seed), 3)
    part_keys = jax.random.split(jax.random.fold_in(key_of[2], part), 3)
    return {
        "tracer": jnp.clip(0.2 + 1.5999999 * jax.random.uniform(part_keys[0], (GRID_J, GRID_I, GRID_K, LEVELS), jnp.float32) ** steps_of(part_keys[0], (GRID_J, GRID_I, GRID_K, LEVELS), ((0, 2), (1, 2), (2, 2)), -0.2, 0.2), 0.2, 1.8),
        "crowding": jnp.clip(0.5 + 1.5 * jax.random.uniform(part_keys[1], (GRID_J, GRID_I, GRID_K, LEVELS), jnp.float32) ** steps_of(part_keys[1], (GRID_J, GRID_I, GRID_K, LEVELS), ((0, 2), (1, 2), (2, 2)), -0.2, 0.2), 0.5, 2.0),
    }


def without_rim(values, dims):
    for dim in dims:
        values = lax.slice_in_dim(values, 1, values.shape[dim] - 1, axis=dim)
    return values


def shifted_cells(values, dim, start, dims):
    others = [other for other in dims if other != dim]
    values = without_rim(values, others)
    return lax.slice_in_dim(values, start, start + values.shape[dim] - 2, axis=dim)


def march_step(padded, crowding):
    middle = without_rim(padded, (0, 1, 2))
    lower = [shifted_cells(padded, dim, 0, (0, 1, 2)) for dim in (0, 1, 2)]
    upper = [shifted_cells(padded, dim, 2, (0, 1, 2)) for dim in (0, 1, 2)]
    spread = lower[0] + upper[0] + lower[1] + upper[1] + lower[2] + upper[2] - 6.0 * middle
    return middle + 0.1 * spread + 0.2 * middle * (1.0 - middle * crowding)


def reference(tracer, crowding):
    for step in range(STEPS):
        tracer = march_step(jnp.pad(tracer, ((1, 1), (1, 1), (1, 1), (0, 0)), mode="constant"), crowding)
    column_sum = jnp.cumsum(tracer, axis=0) / GRID_J
    return column_sum, tracer
```

```python
import functools

import jax
import jax.numpy as jnp
from jax import lax
from jax.experimental import pallas as pl
from jax.experimental.pallas import tpu as pltpu
from jax.sharding import PartitionSpec as P

STEPS = 4
CHUNK = 8
MESH = pl.DeviceIdType.MESH


def kernel(
    sizes,
    tracer_ref,
    crowding_ref,
    column_ref,
    end_ref,
    x,
    crowd,
    sums,
    total,
    below,
    lev_first,
    lev_last,
    lev_lower,
    lev_upper,
    load_sem,
    lat_send,
    lat_recv,
    lon_send,
    lon_recv,
    lev_send,
    lev_recv,
    sum_send,
    sum_recv,
    end_sem,
    column_sem,
):
    J, I, K, L = tracer_ref.shape
    chunks = I // CHUNK
    places = {axis: lax.axis_index(axis) for axis in sizes}
    lower = {axis: places[axis] > 0 for axis in sizes}
    upper = {axis: places[axis] < sizes[axis] - 1 for axis in sizes}

    order = [J - 1, 0] + list(range(1, J - 1))
    loads = []
    for j in order:
        loads.append(pltpu.make_async_copy(tracer_ref.at[j], x.at[0, j + 1, pl.ds(1, I)], load_sem.at[0, j]))
    for j in range(J):
        loads.append(pltpu.make_async_copy(crowding_ref.at[j], crowd.at[j], load_sem.at[1, j]))
    for load in loads:
        load.start()

    barrier = pltpu.get_barrier_semaphore()
    for axis in sizes:
        for there, step in ((lower[axis], -1), (upper[axis], 1)):

            @pl.when(there)
            def _():
                pl.semaphore_signal(barrier, inc=1, device_id={axis: places[axis] + step}, device_id_type=MESH)

    beside = sum(there[axis].astype(jnp.int32) for axis in sizes for there in (lower, upper))
    pl.semaphore_wait(barrier, beside)

    def cells(c):
        return pl.ds(1 + c * CHUNK, CHUNK)

    def lat_copy(r, c, up):
        src, dst = (J, 0) if up else (1, J + 1)
        return pltpu.make_async_remote_copy(
            src_ref=x.at[r, src, cells(c)],
            dst_ref=x.at[r, dst, cells(c)],
            send_sem=lat_send.at[int(up), r, c],
            recv_sem=lat_recv.at[int(up), r, c],
            device_id={"lat": places["lat"] + (1 if up else -1)},
            device_id_type=MESH,
        )

    def lon_copy(r, up):
        src, dst = (I, 0) if up else (1, I + 1)
        return pltpu.make_async_remote_copy(
            src_ref=x.at[r, pl.ds(1, J), src],
            dst_ref=x.at[r, pl.ds(1, J), dst],
            send_sem=lon_send.at[int(up), r],
            recv_sem=lon_recv.at[int(up), r],
            device_id={"lon": places["lon"] + (1 if up else -1)},
            device_id_type=MESH,
        )

    def lev_copy(r, c, up):
        src, dst = (lev_last, lev_lower) if up else (lev_first, lev_upper)
        part = pl.ds(pl.multiple_of(c * CHUNK, CHUNK), CHUNK)
        return pltpu.make_async_remote_copy(
            src_ref=src.at[r, :, part],
            dst_ref=dst.at[r, :, part],
            send_sem=lev_send.at[int(up), r, c],
            recv_sem=lev_recv.at[int(up), r, c],
            device_id={"lev": places["lev"] + (1 if up else -1)},
            device_id_type=MESH,
        )

    def sum_copy(c):
        part = pl.ds(c * CHUNK, CHUNK)
        return pltpu.make_async_remote_copy(
            src_ref=total.at[part],
            dst_ref=below.at[part],
            send_sem=sum_send.at[c],
            recv_sem=sum_recv.at[c],
            device_id={"lat": places["lat"] + 1},
            device_id_type=MESH,
        )

    def end_copy(c):
        return pltpu.make_async_copy(
            x.at[STEPS, pl.ds(1, J), cells(c)], end_ref.at[:, pl.ds(c * CHUNK, CHUNK)], end_sem.at[c]
        )

    def column_copy(c):
        part = pl.ds(c * CHUNK, CHUNK)
        return pltpu.make_async_copy(sums.at[:, part], column_ref.at[:, part], column_sem.at[c])

    def when_do(there, act):
        @pl.when(there)
        def _():
            act()

    def send_lat(r, c):
        when_do(upper["lat"], lambda: lat_copy(r, c, True).start())
        when_do(lower["lat"], lambda: lat_copy(r, c, False).start())

    def send_lev(r, c):
        when_do(upper["lev"], lambda: lev_copy(r, c, True).start())
        when_do(lower["lev"], lambda: lev_copy(r, c, False).start())

    def over(count, body):
        lax.fori_loop(0, count, lambda n, carry: (body(n), carry)[1], 0)

    loads[0].wait()
    when_do(upper["lat"], lambda: over(chunks, lambda c: lat_copy(0, c, True).start()))
    loads[1].wait()
    when_do(lower["lat"], lambda: over(chunks, lambda c: lat_copy(0, c, False).start()))
    for load in loads[2:J]:
        load.wait()
    when_do(upper["lon"], lambda: lon_copy(0, True).start())
    when_do(lower["lon"], lambda: lon_copy(0, False).start())

    def take_edges(c):
        def turn(n):
            i = c * CHUNK + n
            for j in range(J):
                value = x[0, j + 1, i + 1]
                lev_first[0, j, pl.ds(i, 1), :] = value[0:1, :]
                lev_last[0, j, pl.ds(i, 1), :] = value[K - 1 : K, :]

        over(CHUNK, turn)
        send_lev(0, c)

    over(chunks, take_edges)

    def zero_row(row):
        def turn(i):
            x[0, row, i + 1] = jnp.zeros((K, L), jnp.float32)

        over(I, turn)

    def zero_column(column):
        for r in range(STEPS):
            for j in range(J):
                x[r, j + 1, column] = jnp.zeros((K, L), jnp.float32)

    def zero_level(ref):
        for j in range(J):
            ref[0, j] = jnp.zeros((I, L), jnp.float32)

    def zero_below():
        def turn(i):
            below[i] = jnp.zeros((K, L), jnp.float32)

        over(I, turn)

    when_do(jnp.logical_not(lower["lat"]), lambda: zero_row(0))
    when_do(jnp.logical_not(upper["lat"]), lambda: zero_row(J + 1))
    when_do(jnp.logical_not(lower["lon"]), lambda: zero_column(0))
    when_do(jnp.logical_not(upper["lon"]), lambda: zero_column(I + 1))
    when_do(jnp.logical_not(lower["lev"]), lambda: zero_level(lev_lower))
    when_do(jnp.logical_not(upper["lev"]), lambda: zero_level(lev_upper))
    when_do(jnp.logical_not(lower["lat"]), zero_below)
    for load in loads[J:]:
        load.wait()

    level = lax.broadcasted_iota(jnp.int32, (K, L), 0)
    at_first, at_last = level == 0, level == K - 1

    def advance(r, i):
        lat_low = jnp.where(lower["lat"], r, 0)
        lat_high = jnp.where(upper["lat"], r, 0)
        lev_low = jnp.where(lower["lev"], r, 0)
        lev_high = jnp.where(upper["lev"], r, 0)
        rows = [x[lat_low, 0, i + 1]]
        rows += [x[r, j + 1, i + 1] for j in range(J)]
        rows += [x[lat_high, J + 1, i + 1]]
        new = []
        for j in range(J):
            middle = rows[j + 1]
            first = jnp.broadcast_to(lev_lower[lev_low, j, pl.ds(i, 1), :], (K, L))
            last = jnp.broadcast_to(lev_upper[lev_high, j, pl.ds(i, 1), :], (K, L))
            spread = rows[j] + rows[j + 2]
            spread = spread + x[r, j + 1, i] + x[r, j + 1, i + 2]
            spread = spread + jnp.where(at_first, first, pltpu.roll(middle, 1, 0))
            spread = spread + jnp.where(at_last, last, pltpu.roll(middle, K - 1, 0))
            spread = spread - 6.0 * middle
            new.append(middle + 0.1 * spread + 0.2 * middle * (1.0 - middle * crowd[j, i]))
        for j in range(J):
            x[r + 1, j + 1, i + 1] = new[j]
        return new

    def arrive(r, c):
        when_do(lower["lat"], lambda: lat_copy(r, c, True).wait_recv())
        when_do(upper["lat"], lambda: lat_copy(r, c, False).wait_recv())
        when_do(lower["lev"], lambda: lev_copy(r, c, True).wait_recv())
        when_do(upper["lev"], lambda: lev_copy(r, c, False).wait_recv())
        when_do(jnp.logical_and(lower["lon"], c == 0), lambda: lon_copy(r, True).wait_recv())
        when_do(jnp.logical_and(upper["lon"], c == chunks - 1), lambda: lon_copy(r, False).wait_recv())

    def march(n):
        r, c = n // chunks, n % chunks
        arrive(r, c)

        def turn(m):
            i = c * CHUNK + m
            new = advance(r, i)
            for j in range(J):
                lev_first[r + 1, j, pl.ds(i, 1), :] = new[j][0:1, :]
                lev_last[r + 1, j, pl.ds(i, 1), :] = new[j][K - 1 : K, :]

        over(CHUNK, turn)
        send_lat(r + 1, c)
        send_lev(r + 1, c)
        when_do(jnp.logical_and(lower["lon"], c == 0), lambda: lon_copy(r + 1, False).start())
        when_do(jnp.logical_and(upper["lon"], c == chunks - 1), lambda: lon_copy(r + 1, True).start())

    over((STEPS - 1) * chunks, march)

    def finish(c):
        r = STEPS - 1
        arrive(r, c)

        def turn(m):
            i = c * CHUNK + m
            here = None
            for j, value in enumerate(advance(r, i)):
                here = value if here is None else here + value
                sums[j, i] = here
            total[i] = here

        over(CHUNK, turn)
        end_copy(c).start()
        when_do(jnp.logical_not(lower["lat"]), lambda: sum_copy(c).start())

    over(chunks, finish)

    scale = 1.0 / (J * sizes["lat"])

    def conclude(c):
        def pass_on():
            def turn(m):
                i = c * CHUNK + m
                total[i] = total[i] + below[i]

            over(CHUNK, turn)
            sum_copy(c).start()

        when_do(lower["lat"], lambda: sum_copy(c).wait_recv())
        when_do(jnp.logical_and(lower["lat"], upper["lat"]), pass_on)

        def turn(m):
            i = c * CHUNK + m
            before = below[i]
            for j in range(J):
                sums[j, i] = (sums[j, i] + before) * scale

        over(CHUNK, turn)
        column_copy(c).start()

    over(chunks, conclude)

    def sent(n):
        r, c = n // chunks, n % chunks
        when_do(upper["lat"], lambda: lat_copy(r, c, True).wait_send())
        when_do(lower["lat"], lambda: lat_copy(r, c, False).wait_send())
        when_do(upper["lev"], lambda: lev_copy(r, c, True).wait_send())
        when_do(lower["lev"], lambda: lev_copy(r, c, False).wait_send())

    over(STEPS * chunks, sent)

    def sent_lon(r):
        when_do(upper["lon"], lambda: lon_copy(r, True).wait_send())
        when_do(lower["lon"], lambda: lon_copy(r, False).wait_send())

    over(STEPS, sent_lon)

    def ended(c):
        when_do(upper["lat"], lambda: sum_copy(c).wait_send())
        end_copy(c).wait()
        column_copy(c).wait()

    over(chunks, ended)


def on_device(tracer, crowding):
    J, I, K, L = tracer.shape
    sizes = {axis: lax.axis_size(axis) for axis in ("lat", "lon", "lev")}
    chunks = I // CHUNK
    f32, dma = jnp.float32, pltpu.SemaphoreType.DMA
    anywhere = pl.BlockSpec(memory_space=pl.ANY)
    return pl.pallas_call(
        functools.partial(kernel, sizes),
        out_shape=(jax.ShapeDtypeStruct(tracer.shape, f32),) * 2,
        in_specs=[anywhere] * 2,
        out_specs=(anywhere,) * 2,
        scratch_shapes=[
            pltpu.VMEM((STEPS + 1, J + 2, I + 2, K, L), f32),
            pltpu.VMEM((J, I, K, L), f32),
            pltpu.VMEM((J, I, K, L), f32),
            pltpu.VMEM((I, K, L), f32),
            pltpu.VMEM((I, K, L), f32),
            pltpu.VMEM((STEPS, J, I, L), f32),
            pltpu.VMEM((STEPS, J, I, L), f32),
            pltpu.VMEM((STEPS, J, I, L), f32),
            pltpu.VMEM((STEPS, J, I, L), f32),
            dma((2, J)),
            dma((2, STEPS, chunks)),
            dma((2, STEPS, chunks)),
            dma((2, STEPS)),
            dma((2, STEPS)),
            dma((2, STEPS, chunks)),
            dma((2, STEPS, chunks)),
            dma((chunks,)),
            dma((chunks,)),
            dma((chunks,)),
            dma((chunks,)),
        ],
        compiler_params=pltpu.CompilerParams(
            collective_id=0, has_side_effects=True, vmem_limit_bytes=60 * 2**20
        ),
        name="march",
    )(tracer, crowding)


def solution(mesh):
    spec = P(("unit", "lat"), "lon", "lev", None)
    return jax.shard_map(on_device, mesh=mesh, in_specs=(spec, spec), out_specs=(spec, spec), check_vma=False)
```

```python
import functools

import jax
import jax.numpy as jnp
from jax import lax
from jax.experimental import pallas as pl
from jax.experimental.pallas import tpu as pltpu
from jax.sharding import PartitionSpec as P

STEPS = 4
CHUNK = 8
MESH = pl.DeviceIdType.MESH


def kernel(
    sizes,
    tracer_ref,
    crowding_ref,
    sums,
    end,
    x,
    crowd,
    total,
    below,
    lev_first,
    lev_last,
    lev_lower,
    lev_upper,
    load_sem,
    lat_send,
    lat_recv,
    lon_send,
    lon_recv,
    lev_send,
    lev_recv,
    sum_send,
    sum_recv,
):
    J, I, K, L = tracer_ref.shape
    chunks = I // CHUNK
    places = {axis: lax.axis_index(axis) for axis in sizes}
    lower = {axis: places[axis] > 0 for axis in sizes}
    upper = {axis: places[axis] < sizes[axis] - 1 for axis in sizes}

    order = [J - 1, 0] + list(range(1, J - 1))
    loads = []
    for j in order:
        loads.append(pltpu.make_async_copy(tracer_ref.at[j], x.at[0, j + 1, pl.ds(1, I)], load_sem.at[0, j]))
    for j in range(J):
        loads.append(pltpu.make_async_copy(crowding_ref.at[j], crowd.at[j], load_sem.at[1, j]))
    for load in loads[:2]:
        load.start()

    barrier = pltpu.get_barrier_semaphore()
    for axis in sizes:
        for there, step in ((lower[axis], -1), (upper[axis], 1)):

            @pl.when(there)
            def _():
                pl.semaphore_signal(barrier, inc=1, device_id={axis: places[axis] + step}, device_id_type=MESH)

    beside = sum(there[axis].astype(jnp.int32) for axis in sizes for there in (lower, upper))
    pl.semaphore_wait(barrier, beside)

    def cells(c):
        return pl.ds(1 + c * CHUNK, CHUNK)

    def lat_copy(r, c, up):
        src, dst = (J, 0) if up else (1, J + 1)
        return pltpu.make_async_remote_copy(
            src_ref=x.at[r, src, cells(c)],
            dst_ref=x.at[r, dst, cells(c)],
            send_sem=lat_send.at[int(up), r, c],
            recv_sem=lat_recv.at[int(up), r, c],
            device_id={"lat": places["lat"] + (1 if up else -1)},
            device_id_type=MESH,
        )

    def lon_copy(r, up):
        src, dst = (I, 0) if up else (1, I + 1)
        return pltpu.make_async_remote_copy(
            src_ref=x.at[r, pl.ds(1, J), src],
            dst_ref=x.at[r, pl.ds(1, J), dst],
            send_sem=lon_send.at[int(up), r],
            recv_sem=lon_recv.at[int(up), r],
            device_id={"lon": places["lon"] + (1 if up else -1)},
            device_id_type=MESH,
        )

    def lev_copy(r, c, up):
        src, dst = (lev_last, lev_lower) if up else (lev_first, lev_upper)
        part = pl.ds(pl.multiple_of(c * CHUNK, CHUNK), CHUNK)
        return pltpu.make_async_remote_copy(
            src_ref=src.at[r, :, part],
            dst_ref=dst.at[r, :, part],
            send_sem=lev_send.at[int(up), r, c],
            recv_sem=lev_recv.at[int(up), r, c],
            device_id={"lev": places["lev"] + (1 if up else -1)},
            device_id_type=MESH,
        )

    def sum_copy(c):
        part = pl.ds(c * CHUNK, CHUNK)
        return pltpu.make_async_remote_copy(
            src_ref=total.at[part],
            dst_ref=below.at[part],
            send_sem=sum_send.at[c],
            recv_sem=sum_recv.at[c],
            device_id={"lat": places["lat"] + 1},
            device_id_type=MESH,
        )

    def when_do(there, act):
        @pl.when(there)
        def _():
            act()

    def send_lat(r, c):
        when_do(upper["lat"], lambda: lat_copy(r, c, True).start())
        when_do(lower["lat"], lambda: lat_copy(r, c, False).start())

    def send_lev(r, c):
        when_do(upper["lev"], lambda: lev_copy(r, c, True).start())
        when_do(lower["lev"], lambda: lev_copy(r, c, False).start())

    def over(count, body):
        lax.fori_loop(0, count, lambda n, carry: (body(n), carry)[1], 0)

    loads[0].wait()
    when_do(upper["lat"], lambda: over(chunks, lambda c: lat_copy(0, c, True).start()))
    loads[1].wait()
    when_do(lower["lat"], lambda: over(chunks, lambda c: lat_copy(0, c, False).start()))
    for load in loads[2:]:
        load.start()
    for load in loads[2:J]:
        load.wait()
    when_do(upper["lon"], lambda: lon_copy(0, True).start())
    when_do(lower["lon"], lambda: lon_copy(0, False).start())

    def take_edges(c):
        def turn(n):
            i = c * CHUNK + n
            for j in range(J):
                value = x[0, j + 1, i + 1]
                lev_first[0, j, pl.ds(i, 1), :] = value[0:1, :]
                lev_last[0, j, pl.ds(i, 1), :] = value[K - 1 : K, :]

        over(CHUNK, turn)
        send_lev(0, c)

    over(chunks, take_edges)

    def zero_row(row):
        def turn(i):
            x[0, row, i + 1] = jnp.zeros((K, L), jnp.float32)

        over(I, turn)

    def zero_column(column):
        for r in range(STEPS):
            for j in range(J):
                x[r, j + 1, column] = jnp.zeros((K, L), jnp.float32)

    def zero_level(ref):
        for j in range(J):
            ref[0, j] = jnp.zeros((I, L), jnp.float32)

    def zero_below():
        def turn(i):
            below[i] = jnp.zeros((K, L), jnp.float32)

        over(I, turn)

    when_do(jnp.logical_not(lower["lat"]), lambda: zero_row(0))
    when_do(jnp.logical_not(upper["lat"]), lambda: zero_row(J + 1))
    when_do(jnp.logical_not(lower["lon"]), lambda: zero_column(0))
    when_do(jnp.logical_not(upper["lon"]), lambda: zero_column(I + 1))
    when_do(jnp.logical_not(lower["lev"]), lambda: zero_level(lev_lower))
    when_do(jnp.logical_not(upper["lev"]), lambda: zero_level(lev_upper))
    when_do(jnp.logical_not(lower["lat"]), zero_below)
    for load in loads[J:]:
        load.wait()

    level = lax.broadcasted_iota(jnp.int32, (K, L), 0)
    at_first, at_last = level == 0, level == K - 1

    def advance(r, i):
        lat_low = jnp.where(lower["lat"], r, 0)
        lat_high = jnp.where(upper["lat"], r, 0)
        lev_low = jnp.where(lower["lev"], r, 0)
        lev_high = jnp.where(upper["lev"], r, 0)
        rows = [x[lat_low, 0, i + 1]]
        rows += [x[r, j + 1, i + 1] for j in range(J)]
        rows += [x[lat_high, J + 1, i + 1]]
        new = []
        for j in range(J):
            middle = rows[j + 1]
            first = jnp.broadcast_to(lev_lower[lev_low, j, pl.ds(i, 1), :], (K, L))
            last = jnp.broadcast_to(lev_upper[lev_high, j, pl.ds(i, 1), :], (K, L))
            spread = rows[j] + rows[j + 2]
            spread = spread + x[r, j + 1, i] + x[r, j + 1, i + 2]
            spread = spread + jnp.where(at_first, first, pltpu.roll(middle, 1, 0))
            spread = spread + jnp.where(at_last, last, pltpu.roll(middle, K - 1, 0))
            spread = spread - 6.0 * middle
            new.append(middle + 0.1 * spread + 0.2 * middle * (1.0 - middle * crowd[j, i]))
        return new

    def arrive(r, c):
        when_do(lower["lat"], lambda: lat_copy(r, c, True).wait_recv())
        when_do(upper["lat"], lambda: lat_copy(r, c, False).wait_recv())
        when_do(lower["lev"], lambda: lev_copy(r, c, True).wait_recv())
        when_do(upper["lev"], lambda: lev_copy(r, c, False).wait_recv())
        when_do(jnp.logical_and(lower["lon"], c == 0), lambda: lon_copy(r, True).wait_recv())
        when_do(jnp.logical_and(upper["lon"], c == chunks - 1), lambda: lon_copy(r, False).wait_recv())

    def march(n):
        r, c = n // chunks, n % chunks
        arrive(r, c)

        def turn(m):
            i = c * CHUNK + m
            new = advance(r, i)
            for j in range(J):
                x[r + 1, j + 1, i + 1] = new[j]
                lev_first[r + 1, j, pl.ds(i, 1), :] = new[j][0:1, :]
                lev_last[r + 1, j, pl.ds(i, 1), :] = new[j][K - 1 : K, :]

        over(CHUNK, turn)
        send_lat(r + 1, c)
        send_lev(r + 1, c)
        when_do(jnp.logical_and(lower["lon"], c == 0), lambda: lon_copy(r + 1, False).start())
        when_do(jnp.logical_and(upper["lon"], c == chunks - 1), lambda: lon_copy(r + 1, True).start())

    over((STEPS - 1) * chunks, march)

    def finish(c):
        r = STEPS - 1
        arrive(r, c)

        def turn(m):
            i = c * CHUNK + m
            here = None
            for j, value in enumerate(advance(r, i)):
                end[j, i] = value
                here = value if here is None else here + value
                sums[j, i] = here
            total[i] = here

        over(CHUNK, turn)
        when_do(jnp.logical_not(lower["lat"]), lambda: sum_copy(c).start())

    over(chunks, finish)

    scale = 1.0 / (J * sizes["lat"])

    def conclude(c):
        def pass_on():
            def turn(m):
                i = c * CHUNK + m
                total[i] = total[i] + below[i]

            over(CHUNK, turn)
            sum_copy(c).start()

        when_do(lower["lat"], lambda: sum_copy(c).wait_recv())
        when_do(jnp.logical_and(lower["lat"], upper["lat"]), pass_on)

        def turn(m):
            i = c * CHUNK + m
            before = below[i]
            for j in range(J):
                sums[j, i] = (sums[j, i] + before) * scale

        over(CHUNK, turn)

    over(chunks, conclude)

    def sent(n):
        r, c = n // chunks, n % chunks
        when_do(upper["lat"], lambda: lat_copy(r, c, True).wait_send())
        when_do(lower["lat"], lambda: lat_copy(r, c, False).wait_send())
        when_do(upper["lev"], lambda: lev_copy(r, c, True).wait_send())
        when_do(lower["lev"], lambda: lev_copy(r, c, False).wait_send())

    over(STEPS * chunks, sent)

    def sent_lon(r):
        when_do(upper["lon"], lambda: lon_copy(r, True).wait_send())
        when_do(lower["lon"], lambda: lon_copy(r, False).wait_send())

    over(STEPS, sent_lon)

    def ended(c):
        sum_copy(c).wait_send()

    when_do(upper["lat"], lambda: over(chunks, ended))


def write_out(sums, end, column_ref, end_ref, sem):
    copies = []
    for j in range(sums.shape[0]):
        copies.append(pltpu.make_async_copy(sums.at[j], column_ref.at[j], sem.at[0, j]))
        copies.append(pltpu.make_async_copy(end.at[j], end_ref.at[j], sem.at[1, j]))
    for copy in copies:
        copy.start()
    for copy in copies:
        copy.wait()


def on_device(tracer, crowding):
    J, I, K, L = tracer.shape
    sizes = {axis: lax.axis_size(axis) for axis in ("lat", "lon", "lev")}
    chunks = I // CHUNK
    f32, dma = jnp.float32, pltpu.SemaphoreType.DMA
    anywhere = pl.BlockSpec(memory_space=pltpu.HBM)
    inside = pl.BlockSpec(memory_space=pltpu.VMEM)
    results = pl.pallas_call(
        functools.partial(kernel, sizes),
        out_shape=(pltpu.VMEM(tracer.shape, f32),) * 2,
        in_specs=[anywhere] * 2,
        out_specs=(inside,) * 2,
        scratch_shapes=[
            pltpu.VMEM((STEPS, J + 2, I + 2, K, L), f32),
            pltpu.VMEM((J, I, K, L), f32),
            pltpu.VMEM((I, K, L), f32),
            pltpu.VMEM((I, K, L), f32),
            pltpu.VMEM((STEPS, J, I, L), f32),
            pltpu.VMEM((STEPS, J, I, L), f32),
            pltpu.VMEM((STEPS, J, I, L), f32),
            pltpu.VMEM((STEPS, J, I, L), f32),
            dma((2, J)),
            dma((2, STEPS, chunks)),
            dma((2, STEPS, chunks)),
            dma((2, STEPS)),
            dma((2, STEPS)),
            dma((2, STEPS, chunks)),
            dma((2, STEPS, chunks)),
            dma((chunks,)),
            dma((chunks,)),
        ],
        compiler_params=pltpu.CompilerParams(
            collective_id=0, has_side_effects=True, vmem_limit_bytes=52 * 2**20
        ),
        name="march",
    )(tracer, crowding)
    return pl.pallas_call(
        write_out,
        out_shape=(jax.ShapeDtypeStruct(tracer.shape, f32),) * 2,
        in_specs=[inside] * 2,
        out_specs=(anywhere,) * 2,
        scratch_shapes=[dma((2, J))],
        compiler_params=pltpu.CompilerParams(vmem_limit_bytes=2**20),
        name="write_out",
    )(*results)


def solution(mesh):
    spec = P(("unit", "lat"), "lon", "lev", None)
    return jax.shard_map(on_device, mesh=mesh, in_specs=(spec, spec), out_specs=(spec, spec), check_vma=False)
```

```python
import functools

import jax
import jax.numpy as jnp
from jax import lax
from jax.experimental import pallas as pl
from jax.experimental.pallas import tpu as pltpu
from jax.sharding import PartitionSpec as P

STEPS = 4
PIECES = 2
OUT_PIECES = 4
MESH = pl.DeviceIdType.MESH


def kernel(
    sizes,
    tracer_ref,
    crowding_ref,
    end,
    below,
    x,
    crowd,
    total,
    lev_first,
    lev_last,
    lev_lower,
    lev_upper,
    load_sem,
    lat_send,
    lat_recv,
    lon_send,
    lon_recv,
    lev_send,
    lev_recv,
    sum_send,
    sum_recv,
):
    J, I, K, L = tracer_ref.shape
    chunks = PIECES
    CHUNK = I // PIECES
    places = {axis: lax.axis_index(axis) for axis in sizes}
    lower = {axis: places[axis] > 0 for axis in sizes}
    upper = {axis: places[axis] < sizes[axis] - 1 for axis in sizes}

    order = [J - 1, 0] + list(range(1, J - 1))
    loads = []
    for j in order:
        loads.append(pltpu.make_async_copy(tracer_ref.at[j], x.at[0, j + 1, pl.ds(1, I)], load_sem.at[0, j]))
    for j in range(J):
        loads.append(pltpu.make_async_copy(crowding_ref.at[j], crowd.at[j], load_sem.at[1, j]))
    for load in loads[:2]:
        load.start()

    barrier = pltpu.get_barrier_semaphore()
    for axis in sizes:
        for there, step in ((lower[axis], -1), (upper[axis], 1)):

            @pl.when(there)
            def _():
                pl.semaphore_signal(barrier, inc=1, device_id={axis: places[axis] + step}, device_id_type=MESH)

    beside = sum(there[axis].astype(jnp.int32) for axis in sizes for there in (lower, upper))
    pl.semaphore_wait(barrier, beside)

    def cells(c):
        return pl.ds(1 + c * CHUNK, CHUNK)

    def lat_copy(r, c, up):
        src, dst = (J, 0) if up else (1, J + 1)
        return pltpu.make_async_remote_copy(
            src_ref=x.at[r, src, cells(c)],
            dst_ref=x.at[r, dst, cells(c)],
            send_sem=lat_send.at[int(up), r, c],
            recv_sem=lat_recv.at[int(up), r, c],
            device_id={"lat": places["lat"] + (1 if up else -1)},
            device_id_type=MESH,
        )

    def lon_copy(r, up):
        src, dst = (I, 0) if up else (1, I + 1)
        return pltpu.make_async_remote_copy(
            src_ref=x.at[r, pl.ds(1, J), src],
            dst_ref=x.at[r, pl.ds(1, J), dst],
            send_sem=lon_send.at[int(up), r],
            recv_sem=lon_recv.at[int(up), r],
            device_id={"lon": places["lon"] + (1 if up else -1)},
            device_id_type=MESH,
        )

    def lev_copy(r, c, up):
        src, dst = (lev_last, lev_lower) if up else (lev_first, lev_upper)
        part = pl.ds(pl.multiple_of(c * CHUNK, CHUNK), CHUNK)
        return pltpu.make_async_remote_copy(
            src_ref=src.at[r, :, part],
            dst_ref=dst.at[r, :, part],
            send_sem=lev_send.at[int(up), r, c],
            recv_sem=lev_recv.at[int(up), r, c],
            device_id={"lev": places["lev"] + (1 if up else -1)},
            device_id_type=MESH,
        )

    def sum_copy(c):
        part = pl.ds(c * CHUNK, CHUNK)
        return pltpu.make_async_remote_copy(
            src_ref=total.at[part],
            dst_ref=below.at[part],
            send_sem=sum_send.at[c],
            recv_sem=sum_recv.at[c],
            device_id={"lat": places["lat"] + 1},
            device_id_type=MESH,
        )

    def when_do(there, act):
        @pl.when(there)
        def _():
            act()

    def send_lat(r, c):
        when_do(upper["lat"], lambda: lat_copy(r, c, True).start())
        when_do(lower["lat"], lambda: lat_copy(r, c, False).start())

    def send_lev(r, c):
        when_do(upper["lev"], lambda: lev_copy(r, c, True).start())
        when_do(lower["lev"], lambda: lev_copy(r, c, False).start())

    def over(count, body):
        lax.fori_loop(0, count, lambda n, carry: (body(n), carry)[1], 0)

    loads[0].wait()
    when_do(upper["lat"], lambda: over(chunks, lambda c: lat_copy(0, c, True).start()))
    loads[1].wait()
    when_do(lower["lat"], lambda: over(chunks, lambda c: lat_copy(0, c, False).start()))
    for load in loads[2:]:
        load.start()
    for load in loads[2:J]:
        load.wait()
    when_do(upper["lon"], lambda: lon_copy(0, True).start())
    when_do(lower["lon"], lambda: lon_copy(0, False).start())

    def take_edges(c):
        def turn(n):
            i = c * CHUNK + n
            for j in range(J):
                value = x[0, j + 1, i + 1]
                lev_first[0, j, pl.ds(i, 1), :] = value[0:1, :]
                lev_last[0, j, pl.ds(i, 1), :] = value[K - 1 : K, :]

        over(CHUNK, turn)
        send_lev(0, c)

    over(chunks, take_edges)

    def zero_row(row):
        def turn(i):
            x[0, row, i + 1] = jnp.zeros((K, L), jnp.float32)

        over(I, turn)

    def zero_column(column):
        for r in range(STEPS):
            for j in range(J):
                x[r, j + 1, column] = jnp.zeros((K, L), jnp.float32)

    def zero_level(ref):
        for j in range(J):
            ref[0, j] = jnp.zeros((I, L), jnp.float32)

    def zero_below():
        def turn(i):
            below[i] = jnp.zeros((K, L), jnp.float32)

        over(I, turn)

    when_do(jnp.logical_not(lower["lat"]), lambda: zero_row(0))
    when_do(jnp.logical_not(upper["lat"]), lambda: zero_row(J + 1))
    when_do(jnp.logical_not(lower["lon"]), lambda: zero_column(0))
    when_do(jnp.logical_not(upper["lon"]), lambda: zero_column(I + 1))
    when_do(jnp.logical_not(lower["lev"]), lambda: zero_level(lev_lower))
    when_do(jnp.logical_not(upper["lev"]), lambda: zero_level(lev_upper))
    when_do(jnp.logical_not(lower["lat"]), zero_below)
    for load in loads[J:]:
        load.wait()

    level = lax.broadcasted_iota(jnp.int32, (K, L), 0)
    at_first, at_last = level == 0, level == K - 1

    def advance(r, i):
        lat_low = jnp.where(lower["lat"], r, 0)
        lat_high = jnp.where(upper["lat"], r, 0)
        lev_low = jnp.where(lower["lev"], r, 0)
        lev_high = jnp.where(upper["lev"], r, 0)
        rows = [x[lat_low, 0, i + 1]]
        rows += [x[r, j + 1, i + 1] for j in range(J)]
        rows += [x[lat_high, J + 1, i + 1]]
        new = []
        for j in range(J):
            middle = rows[j + 1]
            first = jnp.broadcast_to(lev_lower[lev_low, j, pl.ds(i, 1), :], (K, L))
            last = jnp.broadcast_to(lev_upper[lev_high, j, pl.ds(i, 1), :], (K, L))
            spread = rows[j] + rows[j + 2]
            spread = spread + x[r, j + 1, i] + x[r, j + 1, i + 2]
            spread = spread + jnp.where(at_first, first, pltpu.roll(middle, 1, 0))
            spread = spread + jnp.where(at_last, last, pltpu.roll(middle, K - 1, 0))
            spread = spread - 6.0 * middle
            new.append(middle + 0.1 * spread + 0.2 * middle * (1.0 - middle * crowd[j, i]))
        return new

    def arrive(r, c):
        when_do(lower["lat"], lambda: lat_copy(r, c, True).wait_recv())
        when_do(upper["lat"], lambda: lat_copy(r, c, False).wait_recv())
        when_do(lower["lev"], lambda: lev_copy(r, c, True).wait_recv())
        when_do(upper["lev"], lambda: lev_copy(r, c, False).wait_recv())
        when_do(jnp.logical_and(lower["lon"], c == 0), lambda: lon_copy(r, True).wait_recv())
        when_do(jnp.logical_and(upper["lon"], c == chunks - 1), lambda: lon_copy(r, False).wait_recv())

    def march(n):
        r, c = n // chunks, n % chunks
        arrive(r, c)

        def turn(m):
            i = c * CHUNK + m
            new = advance(r, i)
            for j in range(J):
                x[r + 1, j + 1, i + 1] = new[j]
                lev_first[r + 1, j, pl.ds(i, 1), :] = new[j][0:1, :]
                lev_last[r + 1, j, pl.ds(i, 1), :] = new[j][K - 1 : K, :]

        over(CHUNK, turn)
        send_lat(r + 1, c)
        send_lev(r + 1, c)
        when_do(jnp.logical_and(lower["lon"], c == 0), lambda: lon_copy(r + 1, False).start())
        when_do(jnp.logical_and(upper["lon"], c == chunks - 1), lambda: lon_copy(r + 1, True).start())

    over((STEPS - 1) * chunks, march)

    def finish(c):
        r = STEPS - 1
        arrive(r, c)

        def turn(m):
            i = c * CHUNK + m
            here = None
            for j, value in enumerate(advance(r, i)):
                end[j, i] = value
                here = value if here is None else here + value
            total[i] = here

        over(CHUNK, turn)
        when_do(jnp.logical_not(lower["lat"]), lambda: sum_copy(c).start())

    over(chunks, finish)

    def sent(n):
        r, c = n // chunks, n % chunks
        when_do(upper["lat"], lambda: lat_copy(r, c, True).wait_send())
        when_do(lower["lat"], lambda: lat_copy(r, c, False).wait_send())
        when_do(upper["lev"], lambda: lev_copy(r, c, True).wait_send())
        when_do(lower["lev"], lambda: lev_copy(r, c, False).wait_send())

    over(STEPS * chunks, sent)

    def sent_lon(r):
        when_do(upper["lon"], lambda: lon_copy(r, True).wait_send())
        when_do(lower["lon"], lambda: lon_copy(r, False).wait_send())

    over(STEPS, sent_lon)

    def take_sum(c):
        def pass_on():
            def turn(m):
                i = c * CHUNK + m
                total[i] = total[i] + below[i]

            over(CHUNK, turn)
            sum_copy(c).start()

        sum_copy(c).wait_recv()
        when_do(upper["lat"], pass_on)

    when_do(lower["lat"], lambda: over(chunks, take_sum))
    when_do(upper["lat"], lambda: over(chunks, lambda c: sum_copy(c).wait_send()))


def write_out(scale, end, below, column_ref, end_ref, sums, sem):
    J, I, K, L = end.shape
    length = I // OUT_PIECES

    def end_copy(j):
        return pltpu.make_async_copy(end.at[j], end_ref.at[j], sem.at[0, j])

    def column_copy(c):
        part = pl.ds(c * length, length)
        return pltpu.make_async_copy(sums.at[:, part], column_ref.at[:, part], sem.at[1, c])

    for j in range(J):
        end_copy(j).start()

    def piece(c, carry):
        def turn(m, carry):
            i = c * length + m
            here = below[i]
            for j in range(J):
                here = here + end[j, i]
                sums[j, i] = here * scale
            return carry

        lax.fori_loop(0, length, turn, 0)
        column_copy(c).start()
        return carry

    lax.fori_loop(0, OUT_PIECES, piece, 0)
    for j in range(J):
        end_copy(j).wait()
    for c in range(OUT_PIECES):
        column_copy(c).wait()


def on_device(tracer, crowding):
    J, I, K, L = tracer.shape
    sizes = {axis: lax.axis_size(axis) for axis in ("lat", "lon", "lev")}
    chunks = PIECES
    f32, dma = jnp.float32, pltpu.SemaphoreType.DMA
    anywhere = pl.BlockSpec(memory_space=pltpu.HBM)
    inside = pl.BlockSpec(memory_space=pltpu.VMEM)
    results = pl.pallas_call(
        functools.partial(kernel, sizes),
        out_shape=(pltpu.VMEM(tracer.shape, f32), pltpu.VMEM((I, K, L), f32)),
        in_specs=[anywhere] * 2,
        out_specs=(inside,) * 2,
        scratch_shapes=[
            pltpu.VMEM((STEPS, J + 2, I + 2, K, L), f32),
            pltpu.VMEM((J, I, K, L), f32),
            pltpu.VMEM((I, K, L), f32),
            pltpu.VMEM((STEPS, J, I, L), f32),
            pltpu.VMEM((STEPS, J, I, L), f32),
            pltpu.VMEM((STEPS, J, I, L), f32),
            pltpu.VMEM((STEPS, J, I, L), f32),
            dma((2, J)),
            dma((2, STEPS, chunks)),
            dma((2, STEPS, chunks)),
            dma((2, STEPS)),
            dma((2, STEPS)),
            dma((2, STEPS, chunks)),
            dma((2, STEPS, chunks)),
            dma((chunks,)),
            dma((chunks,)),
        ],
        compiler_params=pltpu.CompilerParams(
            collective_id=0, has_side_effects=True, vmem_limit_bytes=52 * 2**20
        ),
        name="march",
    )(tracer, crowding)
    return pl.pallas_call(
        functools.partial(write_out, 1.0 / (J * sizes["lat"])),
        out_shape=(jax.ShapeDtypeStruct(tracer.shape, f32),) * 2,
        in_specs=[inside] * 2,
        out_specs=(anywhere,) * 2,
        scratch_shapes=[pltpu.VMEM(tracer.shape, f32), dma((2, max(J, OUT_PIECES)))],
        compiler_params=pltpu.CompilerParams(vmem_limit_bytes=8 * 2**20),
        name="write_out",
    )(*results)


def solution(mesh):
    spec = P(("unit", "lat"), "lon", "lev", None)
    return jax.shard_map(on_device, mesh=mesh, in_specs=(spec, spec), out_specs=(spec, spec), check_vma=False)
```

```python
import functools

import jax
import jax.numpy as jnp
from jax import lax
from jax.experimental import pallas as pl
from jax.experimental.pallas import tpu as pltpu
from jax.sharding import PartitionSpec as P

STEPS = 4
PIECES = 2
OUT_PIECES = 4
MESH = pl.DeviceIdType.MESH


def kernel(
    sizes,
    tracer_ref,
    crowding_ref,
    end,
    below,
    x,
    crowd,
    total,
    lev_first,
    lev_last,
    lev_lower,
    lev_upper,
    load_sem,
    lat_send,
    lat_recv,
    lon_send,
    lon_recv,
    lev_send,
    lev_recv,
    sum_send,
    sum_recv,
):
    J, I, K, L = tracer_ref.shape
    chunks = PIECES
    places = {axis: lax.axis_index(axis) for axis in sizes}
    lower = {axis: places[axis] > 0 for axis in sizes}
    upper = {axis: places[axis] < sizes[axis] - 1 for axis in sizes}

    order = [J - 1, 0] + list(range(1, J - 1))
    loads = []
    for j in order:
        loads.append(pltpu.make_async_copy(tracer_ref.at[j], x.at[0, j + 1, pl.ds(1, I)], load_sem.at[0, j]))
    for j in range(J):
        loads.append(pltpu.make_async_copy(crowding_ref.at[j], crowd.at[j], load_sem.at[1, j]))
    for load in loads[:2]:
        load.start()

    barrier = pltpu.get_barrier_semaphore()
    for axis in sizes:
        for there, step in ((lower[axis], -1), (upper[axis], 1)):

            @pl.when(there)
            def _():
                pl.semaphore_signal(barrier, inc=1, device_id={axis: places[axis] + step}, device_id_type=MESH)

    beside = sum(there[axis].astype(jnp.int32) for axis in sizes for there in (lower, upper))
    pl.semaphore_wait(barrier, beside)

    def rounds(length):
        first = (0, length[0])

        def cells(c):
            return pl.ds(1 + first[c], length[c])

        def lat_copy(r, c, up):
            src, dst = (J, 0) if up else (1, J + 1)
            return pltpu.make_async_remote_copy(
                src_ref=x.at[r, src, cells(c)],
                dst_ref=x.at[r, dst, cells(c)],
                send_sem=lat_send.at[int(up), r, c],
                recv_sem=lat_recv.at[int(up), r, c],
                device_id={"lat": places["lat"] + (1 if up else -1)},
                device_id_type=MESH,
            )

        def lon_copy(r, up):
            src, dst = (I, 0) if up else (1, I + 1)
            return pltpu.make_async_remote_copy(
                src_ref=x.at[r, pl.ds(1, J), src],
                dst_ref=x.at[r, pl.ds(1, J), dst],
                send_sem=lon_send.at[int(up), r],
                recv_sem=lon_recv.at[int(up), r],
                device_id={"lon": places["lon"] + (1 if up else -1)},
                device_id_type=MESH,
            )

        def lev_copy(r, c, up):
            src, dst = (lev_last, lev_lower) if up else (lev_first, lev_upper)
            part = pl.ds(first[c], length[c])
            return pltpu.make_async_remote_copy(
                src_ref=src.at[r, :, part],
                dst_ref=dst.at[r, :, part],
                send_sem=lev_send.at[int(up), r, c],
                recv_sem=lev_recv.at[int(up), r, c],
                device_id={"lev": places["lev"] + (1 if up else -1)},
                device_id_type=MESH,
            )

        def sum_copy(c):
            part = pl.ds(first[c], length[c])
            return pltpu.make_async_remote_copy(
                src_ref=total.at[part],
                dst_ref=below.at[part],
                send_sem=sum_send.at[c],
                recv_sem=sum_recv.at[c],
                device_id={"lat": places["lat"] + 1},
                device_id_type=MESH,
            )

        def when_do(there, act):
            @pl.when(there)
            def _():
                act()

        def send_lat(r, c):
            when_do(upper["lat"], lambda: lat_copy(r, c, True).start())
            when_do(lower["lat"], lambda: lat_copy(r, c, False).start())

        def send_lev(r, c):
            when_do(upper["lev"], lambda: lev_copy(r, c, True).start())
            when_do(lower["lev"], lambda: lev_copy(r, c, False).start())

        def each(body):
            for c in range(chunks):
                body(c)

        def over(count, body):
            lax.fori_loop(0, count, lambda n, carry: (body(n), carry)[1], 0)

        loads[0].wait()
        when_do(upper["lat"], lambda: each(lambda c: lat_copy(0, c, True).start()))
        loads[1].wait()
        when_do(lower["lat"], lambda: each(lambda c: lat_copy(0, c, False).start()))
        for load in loads[2:]:
            load.start()
        for load in loads[2:J]:
            load.wait()
        when_do(upper["lon"], lambda: lon_copy(0, True).start())
        when_do(lower["lon"], lambda: lon_copy(0, False).start())

        def take_edges(c):
            def turn(n):
                i = first[c] + n
                for j in range(J):
                    value = x[0, j + 1, i + 1]
                    lev_first[0, j, pl.ds(i, 1), :] = value[0:1, :]
                    lev_last[0, j, pl.ds(i, 1), :] = value[K - 1 : K, :]

            over(length[c], turn)
            send_lev(0, c)

        each(take_edges)

        def zero_row(row):
            def turn(i):
                x[0, row, i + 1] = jnp.zeros((K, L), jnp.float32)

            over(I, turn)

        def zero_column(column):
            for r in range(STEPS):
                for j in range(J):
                    x[r, j + 1, column] = jnp.zeros((K, L), jnp.float32)

        def zero_level(ref):
            for j in range(J):
                ref[0, j] = jnp.zeros((I, L), jnp.float32)

        def zero_below():
            def turn(i):
                below[i] = jnp.zeros((K, L), jnp.float32)

            over(I, turn)

        when_do(jnp.logical_not(lower["lat"]), lambda: zero_row(0))
        when_do(jnp.logical_not(upper["lat"]), lambda: zero_row(J + 1))
        when_do(jnp.logical_not(lower["lon"]), lambda: zero_column(0))
        when_do(jnp.logical_not(upper["lon"]), lambda: zero_column(I + 1))
        when_do(jnp.logical_not(lower["lev"]), lambda: zero_level(lev_lower))
        when_do(jnp.logical_not(upper["lev"]), lambda: zero_level(lev_upper))
        when_do(jnp.logical_not(lower["lat"]), zero_below)
        for load in loads[J:]:
            load.wait()

        level = lax.broadcasted_iota(jnp.int32, (K, L), 0)
        at_first, at_last = level == 0, level == K - 1

        def advance(r, i):
            lat_low = jnp.where(lower["lat"], r, 0)
            lat_high = jnp.where(upper["lat"], r, 0)
            lev_low = jnp.where(lower["lev"], r, 0)
            lev_high = jnp.where(upper["lev"], r, 0)
            rows = [x[lat_low, 0, i + 1]]
            rows += [x[r, j + 1, i + 1] for j in range(J)]
            rows += [x[lat_high, J + 1, i + 1]]
            new = []
            for j in range(J):
                middle = rows[j + 1]
                first = jnp.broadcast_to(lev_lower[lev_low, j, pl.ds(i, 1), :], (K, L))
                last = jnp.broadcast_to(lev_upper[lev_high, j, pl.ds(i, 1), :], (K, L))
                spread = rows[j] + rows[j + 2]
                spread = spread + x[r, j + 1, i] + x[r, j + 1, i + 2]
                spread = spread + jnp.where(at_first, first, pltpu.roll(middle, 1, 0))
                spread = spread + jnp.where(at_last, last, pltpu.roll(middle, K - 1, 0))
                spread = spread - 6.0 * middle
                new.append(middle + 0.1 * spread + 0.2 * middle * (1.0 - middle * crowd[j, i]))
            return new

        def arrive(r, c):
            when_do(lower["lat"], lambda: lat_copy(r, c, True).wait_recv())
            when_do(upper["lat"], lambda: lat_copy(r, c, False).wait_recv())
            when_do(lower["lev"], lambda: lev_copy(r, c, True).wait_recv())
            when_do(upper["lev"], lambda: lev_copy(r, c, False).wait_recv())
            c == 0 and when_do(lower["lon"], lambda: lon_copy(r, True).wait_recv())
            c == chunks - 1 and when_do(upper["lon"], lambda: lon_copy(r, False).wait_recv())

        def march(r, c):
            arrive(r, c)

            def turn(m):
                i = first[c] + m
                new = advance(r, i)
                for j in range(J):
                    x[r + 1, j + 1, i + 1] = new[j]
                    lev_first[r + 1, j, pl.ds(i, 1), :] = new[j][0:1, :]
                    lev_last[r + 1, j, pl.ds(i, 1), :] = new[j][K - 1 : K, :]

            over(length[c], turn)
            send_lat(r + 1, c)
            send_lev(r + 1, c)
            c == 0 and when_do(lower["lon"], lambda: lon_copy(r + 1, False).start())
            c == chunks - 1 and when_do(upper["lon"], lambda: lon_copy(r + 1, True).start())

        over(STEPS - 1, lambda r: each(lambda c: march(r, c)))

        def finish(c):
            r = STEPS - 1
            arrive(r, c)

            def turn(m):
                i = first[c] + m
                here = None
                for j, value in enumerate(advance(r, i)):
                    end[j, i] = value
                    here = value if here is None else here + value
                total[i] = here

            over(length[c], turn)
            when_do(jnp.logical_not(lower["lat"]), lambda: sum_copy(c).start())

        each(finish)

        def sent(r, c):
            when_do(upper["lat"], lambda: lat_copy(r, c, True).wait_send())
            when_do(lower["lat"], lambda: lat_copy(r, c, False).wait_send())
            when_do(upper["lev"], lambda: lev_copy(r, c, True).wait_send())
            when_do(lower["lev"], lambda: lev_copy(r, c, False).wait_send())

        over(STEPS, lambda r: each(lambda c: sent(r, c)))

        def sent_lon(r):
            when_do(upper["lon"], lambda: lon_copy(r, True).wait_send())
            when_do(lower["lon"], lambda: lon_copy(r, False).wait_send())

        over(STEPS, sent_lon)

        def take_sum(c):
            def pass_on():
                def turn(m):
                    i = first[c] + m
                    total[i] = total[i] + below[i]

                over(length[c], turn)
                sum_copy(c).start()

            sum_copy(c).wait_recv()
            when_do(upper["lat"], pass_on)

        when_do(lower["lat"], lambda: each(take_sum))
        when_do(upper["lat"], lambda: each(lambda c: sum_copy(c).wait_send()))

    short = I // 8 * 3

    @pl.when(places["lon"] % 2 == 0)
    def _():
        rounds((I - short, short))

    @pl.when(places["lon"] % 2 == 1)
    def _():
        rounds((short, I - short))


def write_out(scale, end, below, column_ref, end_ref, sums, sem):
    J, I, K, L = end.shape
    length = I // OUT_PIECES

    def end_copy(j):
        return pltpu.make_async_copy(end.at[j], end_ref.at[j], sem.at[0, j])

    def column_copy(c):
        part = pl.ds(c * length, length)
        return pltpu.make_async_copy(sums.at[:, part], column_ref.at[:, part], sem.at[1, c])

    for j in range(J):
        end_copy(j).start()

    def piece(c, carry):
        def turn(m, carry):
            i = c * length + m
            here = below[i]
            for j in range(J):
                here = here + end[j, i]
                sums[j, i] = here * scale
            return carry

        lax.fori_loop(0, length, turn, 0)
        column_copy(c).start()
        return carry

    lax.fori_loop(0, OUT_PIECES, piece, 0)
    for j in range(J):
        end_copy(j).wait()
    for c in range(OUT_PIECES):
        column_copy(c).wait()


def on_device(tracer, crowding):
    J, I, K, L = tracer.shape
    sizes = {axis: lax.axis_size(axis) for axis in ("lat", "lon", "lev")}
    chunks = PIECES
    f32, dma = jnp.float32, pltpu.SemaphoreType.DMA
    anywhere = pl.BlockSpec(memory_space=pltpu.HBM)
    inside = pl.BlockSpec(memory_space=pltpu.VMEM)
    results = pl.pallas_call(
        functools.partial(kernel, sizes),
        out_shape=(pltpu.VMEM(tracer.shape, f32), pltpu.VMEM((I, K, L), f32)),
        in_specs=[anywhere] * 2,
        out_specs=(inside,) * 2,
        scratch_shapes=[
            pltpu.VMEM((STEPS, J + 2, I + 2, K, L), f32),
            pltpu.VMEM((J, I, K, L), f32),
            pltpu.VMEM((I, K, L), f32),
            pltpu.VMEM((STEPS, J, I, L), f32),
            pltpu.VMEM((STEPS, J, I, L), f32),
            pltpu.VMEM((STEPS, J, I, L), f32),
            pltpu.VMEM((STEPS, J, I, L), f32),
            dma((2, J)),
            dma((2, STEPS, chunks)),
            dma((2, STEPS, chunks)),
            dma((2, STEPS)),
            dma((2, STEPS)),
            dma((2, STEPS, chunks)),
            dma((2, STEPS, chunks)),
            dma((chunks,)),
            dma((chunks,)),
        ],
        compiler_params=pltpu.CompilerParams(
            collective_id=0, has_side_effects=True, vmem_limit_bytes=52 * 2**20
        ),
        name="march",
    )(tracer, crowding)
    return pl.pallas_call(
        functools.partial(write_out, 1.0 / (J * sizes["lat"])),
        out_shape=(jax.ShapeDtypeStruct(tracer.shape, f32),) * 2,
        in_specs=[inside] * 2,
        out_specs=(anywhere,) * 2,
        scratch_shapes=[pltpu.VMEM(tracer.shape, f32), dma((2, max(J, OUT_PIECES)))],
        compiler_params=pltpu.CompilerParams(vmem_limit_bytes=8 * 2**20),
        name="write_out",
    )(*results)


def solution(mesh):
    spec = P(("unit", "lat"), "lon", "lev", None)
    return jax.shard_map(on_device, mesh=mesh, in_specs=(spec, spec), out_specs=(spec, spec), check_vma=False)
```
